256 devices in a mesh: section: 4 (over y), seq: 64 (over z, x, core).
Axes of the slice: x: 4, y: 4, z: 8, core: 2. Of those that a mesh axis runs over, the one named last changes fastest.
Arguments:
- patches: bfloat16 [64, 729, 1152], P('seq'), may hold values from -40 to 40
- fc_gain: float32 [4, 1152], P('section'), may hold values from 0.1 to 1.9
- fc_in: bfloat16 [4, 1152, 2176], P('section', 'seq'), may hold values from -0.1875 to 0.1875
- fc_in_bias: float32 [4, 2176], P('section'), may hold values from -3 to 3
- fc_out: bfloat16 [4, 2176, 1152], P('section', None, 'seq'), may hold values from -0.125 to 0.125
- fc_out_bias: float32 [4, 1152], P('section'), may hold values from -3 to 3
- proj_weight: bfloat16 [1152, 3584], P('seq'), may hold values from -0.1875 to 0.1875
- text_embed: bfloat16 [8192, 3584], P('seq'), may hold values from -40 to 40
- frame_start: int32 [64], replicated, may hold values from 0 to 8191, as said below
- frame_count: int32 [64], replicated, may hold values from 1 to 196, as said below
- segment_ids: int32 [8192], replicated, may hold values from 0 to 2, as said below
- norm_gain: float32 [3584], replicated, may hold values from 0.1 to 1.9
- query_weight: bfloat16 [3584, 2048], P(None, 'section'), may hold values from -3 to 3
- query_bias: float32 [2048], P('section'), may hold values from -3 to 3
- key_weight: bfloat16 [3584, 512], P(None, 'section'), may hold values from -1 to 1
- value_weight: bfloat16 [3584, 512], P(None, 'section'), may hold values from -0.09375 to 0.09375
- value_bias: float32 [512], P('section'), may hold values from -3 to 3
Outputs:
- attended: bfloat16 [8192, 2048], P('seq', 'section')
The draws below stay inside these ranges and needn't reach their ends.
Inputs may be any that keep to these rules, and one draw needn't show every extreme that they name: Frame f keeps its first frame_count[f] pooled tokens and places them at positions frame_start[f] to frame_start[f] + frame_count[f] - 1; frame f begins in shard f, at a position from f * 128 to (f + 1) * 128 - 1; every frame ends before the next one begins, and the last ends by position 8191. The frame of shard 64 / 2 - 1 runs into the next shard. `frame_count`: some frame keeps all 196 tokens. `segment_ids`: segment numbers never fall along the sequence, and each of 0, 1 and 2 occurs.
All inputs are finite; a program needn't handle non-finite values.
Results may differ from the reference program's by a relative error of at most 0.02.
Values may be sent and summed in bfloat16 or wider, within the bound.
No kernel may reach another device: no remote copies, remote signals or barrier semaphores. Data moves between devices by JAX's collectives and lax.ppermute only.
A program may use at most 128 MiB of HBM per device.

```python
import math
import jax
import jax.numpy as jnp
from jax import lax

D = 1152
FF = 2176
GRID = 27
HM = 3584
HEAD = 128
KV_HEADS = 4
QPK = 4
L_DEV = 128
PATCH = 729
POOLED = 196
QHEADS = 16
LAYERS = 4
FRAMES = 64
L_TOTAL = 8192
N_SEQ = 64


def rough_field(key, lead_shape, feature_width):
    k_base, k_rows, k_cols = jax.random.split(key, 3)
    base_draw = jax.random.normal(k_base, lead_shape + (feature_width,), jnp.float32)
    base_draw = jnp.clip(base_draw, -4.0, 4.0)
    row_scale = jnp.exp(jax.random.uniform(k_rows, lead_shape + (1,), jnp.float32, -1.15, 1.15))
    col_scale = jnp.exp(jax.random.uniform(k_cols, (feature_width,), jnp.float32, -1.15, 1.15))
    return base_draw * row_scale * col_scale


def draw_patches(key, part):
    return rough_field(jax.random.fold_in(key, 3), (FRAMES, PATCH), D).astype(jnp.bfloat16)


def draw_text_embed(key, part):
    return rough_field(jax.random.fold_in(key, 4), (L_TOTAL,), HM).astype(jnp.bfloat16)


def attention_pair(key):
    k_keys, k_noise = jax.random.split(jax.random.fold_in(key, 7), 2)
    root_width = math.sqrt(HM)
    key_draw = jnp.clip(jax.random.normal(k_keys, (HM, KV_HEADS, 1, HEAD), jnp.float32), -6.0, 6.0) / root_width
    noise_draw = jnp.clip(jax.random.normal(k_noise, (HM, KV_HEADS, QPK, HEAD), jnp.float32), -6.0, 6.0) * (3.5 / root_width)
    queries = noise_draw
    queries = jnp.clip(queries, -3.0, 3.0).reshape(HM, KV_HEADS * QPK * HEAD)
    return (key_draw.reshape(HM, KV_HEADS * HEAD), queries)


def draw_query_weight(key, part):
    return attention_pair(key)[1].astype(jnp.bfloat16)


def draw_key_weight(key, part):
    return attention_pair(key)[0].astype(jnp.bfloat16)


def frame_layout(key):
    k_offsets, k_chosen, k_counts = jax.random.split(jax.random.fold_in(key, 13), 3)
    middle = FRAMES // 2 - 1
    offsets = jax.random.randint(k_offsets, (FRAMES,), 0, L_DEV)
    chosen = jax.random.randint(k_chosen, (), 0, FRAMES - 4)
    chosen = jnp.where(chosen >= middle - 1, chosen + 3, chosen)
    frame_index = jnp.arange(FRAMES)
    offsets = jnp.where(frame_index == chosen, 0, offsets)
    offsets = jnp.where(frame_index == chosen + 1, max(POOLED - L_DEV, 0), offsets)
    offsets = jnp.where((frame_index == middle) | (frame_index == middle + 1), L_DEV - 1, offsets)
    following = jnp.concatenate([offsets[1:], jnp.zeros((1,), offsets.dtype)])
    upper_limit = jnp.minimum(POOLED, L_DEV + following - offsets)
    upper_limit = jnp.where(frame_index == FRAMES - 1, jnp.minimum(POOLED, L_DEV - offsets), upper_limit)
    lower_limit = jnp.maximum(1, upper_limit // 2)
    counts = jax.random.randint(k_counts, (FRAMES,), lower_limit, upper_limit + 1)
    counts = jnp.where(frame_index == chosen, POOLED, counts)
    counts = jnp.where(frame_index == middle, upper_limit, counts)
    starts = frame_index * L_DEV + offsets
    return (starts.astype(jnp.int32), counts.astype(jnp.int32))


def draw_frame_start(key, part):
    return frame_layout(key)[0]


def draw_frame_count(key, part):
    return frame_layout(key)[1]


def draw_segment_ids(key, part):
    k_first, k_second = jax.random.split(jax.random.fold_in(key, 5))
    first_cut = jax.random.randint(k_first, (), L_TOTAL // 16, L_TOTAL // 8)
    second_cut = jax.random.randint(k_second, (), L_TOTAL // 8, L_TOTAL // 4)
    positions = jnp.arange(L_TOTAL)
    return ((positions >= first_cut).astype(jnp.int32) + (positions >= second_cut).astype(jnp.int32)).astype(jnp.int32)


def block_levels(own_key, dims, cuts, least, largest):
    def one(position, parts):
        draws = jax.random.uniform(jax.random.fold_in(jax.random.fold_in(own_key, 6), position), (parts,), jnp.float32, least / len(cuts), largest / len(cuts))
        return jnp.repeat(jnp.exp(draws), dims[position] // parts).reshape((-1,) + (1,) * (len(dims) - position - 1))

    gain = one(*cuts[0])
    for cut in cuts[1:]:
        gain = gain * one(*cut)
    return gain


def noise(rng, dims, deviation, reach, pieces=(), kind=jnp.bfloat16):
    gain = block_levels(rng, dims, pieces, -0.22, 0.18) if pieces else 1.0
    array = jax.random.normal(rng, dims, jnp.float32) * deviation * gain
    return jnp.minimum(jnp.maximum(array, -reach), reach).astype(kind)


def setup_inputs(seed: int = 0) -> dict:
    arg_keys = jax.random.split(jax.random.key(seed), 18)
    patches = draw_patches(jax.random.fold_in(arg_keys[17], 71), 0)
    fc_gain = jnp.clip(1.0 + 0.18 * jax.random.normal(arg_keys[1], (LAYERS, D), jnp.float32), 0.1, 1.9)
    fc_in = noise(arg_keys[2], (LAYERS, D, FF), D ** -0.5, 0.1875, ((0, 4), (1, 64)))
    fc_in_bias = noise(arg_keys[3], (LAYERS, FF), 0.5, 3.0, ((0, 4),), jnp.float32)
    fc_out = noise(arg_keys[4], (LAYERS, FF, D), FF ** -0.5, 0.125, ((0, 4), (2, 64)))
    fc_out_bias = noise(arg_keys[5], (LAYERS, D), 0.5, 3.0, ((0, 4),), jnp.float32)
    proj_weight = noise(arg_keys[6], (D, HM), D ** -0.5, 0.1875, ((0, 64),))
    text_embed = draw_text_embed(jax.random.fold_in(arg_keys[17], 71), 0)
    frame_start = draw_frame_start(jax.random.fold_in(arg_keys[17], 71), 0)
    frame_count = draw_frame_count(jax.random.fold_in(arg_keys[17], 71), 0)
    segment_ids = draw_segment_ids(jax.random.fold_in(arg_keys[17], 71), 0)
    norm_gain = jnp.clip(1.0 + 0.18 * jax.random.normal(arg_keys[11], (HM,), jnp.float32), 0.1, 1.9)
    query_weight = draw_query_weight(jax.random.fold_in(arg_keys[17], 71), 0)
    query_bias = noise(arg_keys[13], (QHEADS * HEAD,), 0.5, 3.0, ((0, 4),), jnp.float32)
    key_weight = draw_key_weight(jax.random.fold_in(arg_keys[17], 71), 0)
    value_weight = noise(arg_keys[15], (HM, KV_HEADS * HEAD), HM ** -0.5, 0.09375, ((1, 4),))
    value_bias = noise(arg_keys[16], (KV_HEADS * HEAD,), 0.5, 3.0, ((0, 4),), jnp.float32)
    return {"patches": patches, "fc_gain": fc_gain, "fc_in": fc_in, "fc_in_bias": fc_in_bias, "fc_out": fc_out, "fc_out_bias": fc_out_bias, "proj_weight": proj_weight, "text_embed": text_embed, "frame_start": frame_start, "frame_count": frame_count, "segment_ids": segment_ids, "norm_gain": norm_gain, "query_weight": query_weight, "query_bias": query_bias, "key_weight": key_weight, "value_weight": value_weight, "value_bias": value_bias}


layer_eps = 1e-06
rms_eps = 1e-06
rope_base = 1000000.0

def layer_norm(values, scales):
    widened = values.astype(jnp.float32)
    center = widened - lax.optimization_barrier(jnp.mean(widened, axis=-1, keepdims=True))
    spread = lax.optimization_barrier(jnp.mean(center * center, axis=-1, keepdims=True))
    return center * lax.rsqrt(spread + layer_eps) * scales

def encoder_layer(values, scales, w_in, b_in, w_out, b_out):
    normed = layer_norm(values, scales).astype(jnp.bfloat16)
    hidden = jax.nn.gelu(jnp.dot(normed, w_in, preferred_element_type=jnp.float32) + b_in, approximate=True).astype(jnp.bfloat16)
    summed = values.astype(jnp.float32) + jnp.dot(hidden, w_out, preferred_element_type=jnp.float32) + b_out
    return summed.astype(jnp.bfloat16)

def pool_frame(encoded):
    lead_dims = encoded.shape[:-2]
    channel = encoded.shape[-1]
    grid_side = GRID
    pool_side = (GRID + 1) // 2
    grid_cells = encoded.astype(jnp.float32).reshape(lead_dims + (grid_side, grid_side, channel))
    pad_cells = 2 * pool_side - grid_side
    grid_cells = jnp.pad(grid_cells, [(0, 0)] * len(lead_dims) + [(0, pad_cells), (0, pad_cells), (0, 0)])
    totals = grid_cells.reshape(lead_dims + (pool_side, 2, pool_side, 2, channel)).sum(axis=(-4, -2))
    counts = jnp.minimum(2, grid_side - 2 * jnp.arange(pool_side)).astype(jnp.float32)
    cell_area = counts[:, None] * counts[None, :]
    return (totals / cell_area[..., None]).reshape(lead_dims + (pool_side * pool_side, channel))

def rotate(values, positions):
    head_dim = values.shape[-1]
    half_dim = head_dim // 2
    inv_rates = jnp.exp(jnp.arange(half_dim, dtype=jnp.float32) * (-2.0 * math.log(rope_base) / head_dim))
    angles = positions.astype(jnp.float32)[:, None] * inv_rates[None, :]
    cosine = jnp.cos(angles)[:, None, :]
    sine_part = jnp.sin(angles)[:, None, :]
    first_half = values[..., :half_dim]
    second = values[..., half_dim:]
    return jnp.concatenate([first_half * cosine - second * sine_part, second * cosine + first_half * sine_part], axis=-1)

def reference(patches, fc_gain, fc_in, fc_in_bias, fc_out, fc_out_bias, proj_weight, text_embed, frame_start, frame_count, segment_ids, norm_gain, query_weight, query_bias, key_weight, value_weight, value_bias):
    encoded = patches.reshape(FRAMES * PATCH, D)
    for layer_index in range(LAYERS):
        encoded = encoder_layer(encoded, fc_gain[layer_index], fc_in[layer_index], fc_in_bias[layer_index], fc_out[layer_index], fc_out_bias[layer_index])
    pooled = pool_frame(encoded.reshape(FRAMES, PATCH, D)).astype(jnp.bfloat16)
    projected = jnp.dot(pooled.reshape(FRAMES * POOLED, D), proj_weight, preferred_element_type=jnp.float32).astype(jnp.bfloat16)
    positions = jnp.arange(L_TOTAL, dtype=jnp.int32)
    home_frame = (positions // L_DEV).astype(jnp.int32)
    before = jnp.maximum(home_frame - 1, 0).astype(jnp.int32)

    def pick_tokens(frame_ids, ok_extra):
        offset = positions - frame_start[frame_ids]
        is_valid = ok_extra & (offset >= 0) & (offset < frame_count[frame_ids])
        picked = jnp.take(projected, frame_ids * POOLED + jnp.clip(offset, 0, POOLED - 1), axis=0)
        return (is_valid, picked)
    own_valid, own_rows = pick_tokens(home_frame, True)
    prev_valid, prev_rows = pick_tokens(before, home_frame > 0)
    inputs = jnp.where(own_valid[:, None], own_rows, jnp.where(prev_valid[:, None], prev_rows, text_embed))
    widened = inputs.astype(jnp.float32)
    normed = (widened * lax.rsqrt(lax.optimization_barrier(jnp.mean(widened * widened, axis=-1, keepdims=True)) + rms_eps) * norm_gain).astype(jnp.bfloat16)
    queries = jnp.dot(normed, query_weight, preferred_element_type=jnp.float32) + query_bias
    queries = rotate(queries.reshape(L_TOTAL, KV_HEADS * QPK, HEAD), positions).astype(jnp.bfloat16)
    key_heads = jnp.dot(normed, key_weight, preferred_element_type=jnp.float32)
    key_heads = rotate(key_heads.reshape(L_TOTAL, KV_HEADS, HEAD), positions).astype(jnp.bfloat16)
    values = (jnp.dot(normed, value_weight, preferred_element_type=jnp.float32) + value_bias).astype(jnp.bfloat16)
    values = values.reshape(L_TOTAL, KV_HEADS, HEAD)
    key_float = key_heads.astype(jnp.float32)
    value_float = values.astype(jnp.float32)
    score_scale = 1.0 / math.sqrt(HEAD)

    def attend_rows(block_index):
        row_start = (block_index * L_DEV).astype(jnp.int32)
        query_rows = lax.dynamic_slice_in_dim(queries, row_start, L_DEV, 0).astype(jnp.float32)
        query_rows = query_rows.reshape(L_DEV, KV_HEADS, QPK, HEAD)
        query_pos = row_start + jnp.arange(L_DEV, dtype=jnp.int32)
        query_seg = lax.dynamic_slice_in_dim(segment_ids, row_start, L_DEV, 0)
        scores = jnp.einsum('qgjd,kgd->gjqk', query_rows, key_float) * score_scale
        allowed = (positions[None, :] <= query_pos[:, None]) & (segment_ids[None, :] == query_seg[:, None])
        row_top = lax.optimization_barrier(jnp.max(jnp.where(allowed, scores, -jnp.inf), axis=-1, keepdims=True))
        weights = jnp.where(allowed, jnp.exp(scores - row_top), 0.0)
        row_total = lax.optimization_barrier(jnp.sum(weights, axis=-1))
        rounded = lax.optimization_barrier(weights.astype(jnp.bfloat16)).astype(jnp.float32)
        mixed = jnp.einsum('gjqk,kgd->qgjd', rounded, value_float)
        mixed = mixed / jnp.transpose(row_total, (2, 0, 1))[..., None]
        return mixed.reshape(L_DEV, KV_HEADS * QPK * HEAD).astype(jnp.bfloat16)
    attended = lax.map(attend_rows, jnp.arange(N_SEQ, dtype=jnp.int32))
    return attended.reshape(L_TOTAL, KV_HEADS * QPK * HEAD)
```

```python
import math

import jax
import jax.numpy as jnp
from jax import lax
from jax.experimental import pallas as pl
from jax.experimental.pallas import tpu as pltpu
from jax.sharding import Mesh, PartitionSpec as P

GRID = 27
POOL = 14
D = 1152
FF = 2176
HM = 3584
HEAD = 128
QPK = 4
L_DEV = 128
N_SEQ = 64
MAIN = 1024
LEFT = 128
LAYER_COLS = 2 * FF
HALF_ROWS = POOL * GRID
CHUNK_ROWS = HALF_ROWS // 2
FF_CUTS = (0, 512, 1024, 1536, 2176)

layer_eps = 1e-06
rms_eps = 1e-06
rope_base = 1000000.0
mask_floor = -1e30

SEQ = ("z", "x", "core")


def fold_rows(shard):
    width = shard.shape[1]
    piece = -(-width // (8 * 128)) * 128
    rest = jnp.pad(shard[16:], ((0, 0), (0, 8 * piece - width)))
    return shard[:16], rest.reshape(16, piece)


def unfold_rows(gathered, width):
    piece = gathered.shape[1]
    return gathered.reshape(N_SEQ * 2, 8 * piece)[:, :width]


def feature_order(v):
    split = v.reshape(v.shape[:-1] + (N_SEQ, 18))
    main = split[..., :16].reshape(v.shape[:-1] + (MAIN,))
    left = split[..., 16:].reshape(v.shape[:-1] + (LEFT,))
    return jnp.concatenate([main, left], axis=-1)


def order_matrix():
    to = jnp.arange(D)
    low = (to // 16) * 18 + to % 16
    rest = to - MAIN
    high = (rest // 2) * 18 + 16 + rest % 2
    source = jnp.where(to < MAIN, low, high)
    return (jnp.arange(D)[:, None] == source[None, :]).astype(jnp.bfloat16)


def encoder_kernel(x_ref, gain_ref, bin_ref, bout_ref, left_ref, full_ref, out_ref, w_in, w_out, sems):
    cuts = list(zip(FF_CUTS[:-1], FF_CUTS[1:]))
    copies = []
    for layer in range(2):
        base = layer * LAYER_COLS
        for index, (lo, hi) in enumerate(cuts):
            pair = []
            for kind, (buf, shift) in enumerate(((w_in, 0), (w_out, FF))):
                copy = pltpu.make_async_copy(
                    full_ref.at[:, base + shift + lo : base + shift + hi],
                    buf.at[layer, :, lo:hi],
                    sems.at[layer, index, kind],
                )
                copy.start()
                pair.append(copy)
            copies.append(pair)

    x = x_ref[...].astype(jnp.float32)
    for layer in range(2):
        base = layer * LAYER_COLS
        center = x - jnp.mean(x, axis=1, keepdims=True)
        spread = jnp.mean(center * center, axis=1, keepdims=True)
        normed = (center * lax.rsqrt(spread + layer_eps) * gain_ref[layer : layer + 1, :]).astype(jnp.bfloat16)
        acc_main = jnp.zeros((x.shape[0], MAIN), jnp.float32)
        acc_left = jnp.zeros((x.shape[0], LEFT), jnp.float32)
        for index, (lo, hi) in enumerate(cuts):
            copy_in, copy_out = copies[layer * len(cuts) + index]
            copy_in.wait()
            pre = jnp.dot(normed[:, :MAIN], w_in[layer, :, lo:hi], preferred_element_type=jnp.float32)
            pre = pre + jnp.dot(
                normed[:, MAIN:], left_ref[:, base + lo : base + hi], preferred_element_type=jnp.float32
            )
            hidden = jax.nn.gelu(pre + bin_ref[layer : layer + 1, lo:hi], approximate=True).astype(jnp.bfloat16)
            copy_out.wait()
            last = (((1,), (1,)), ((), ()))
            acc_main = acc_main + lax.dot_general(
                hidden, w_out[layer, :, lo:hi], last, preferred_element_type=jnp.float32
            )
            acc_left = acc_left + lax.dot_general(
                hidden, left_ref[:, base + FF + lo : base + FF + hi], last, preferred_element_type=jnp.float32
            )
        x = x + jnp.concatenate([acc_main, acc_left], axis=1) + bout_ref[layer : layer + 1, :]
        x = x.astype(jnp.bfloat16).astype(jnp.float32)
    out_ref[...] = x.astype(jnp.bfloat16)


def encode(x, gain, b_in, b_out, left, full):
    vmem = pl.BlockSpec(memory_space=pltpu.VMEM)
    return pl.pallas_call(
        encoder_kernel,
        out_shape=jax.ShapeDtypeStruct(x.shape, jnp.bfloat16),
        in_specs=[vmem, vmem, vmem, vmem, vmem, pl.BlockSpec(memory_space=pl.ANY)],
        out_specs=vmem,
        scratch_shapes=[
            pltpu.VMEM((2, MAIN, FF), jnp.bfloat16),
            pltpu.VMEM((2, MAIN, FF), jnp.bfloat16),
            pltpu.SemaphoreType.DMA((2, len(FF_CUTS) - 1, 2)),
        ],
        compiler_params=pltpu.CompilerParams(vmem_limit_bytes=44 * 1024 * 1024),
        name="encoder_pair",
    )(x, gain, b_in, b_out, left, full)


def attend_kernel(info_ref, q_ref, low_ref, *rest):
    pieces, (out_ref, keys, turned, acc, top, total, sems) = rest[:10], rest[10:]
    copies, at = [], 0
    for index, piece in enumerate(pieces):
        count = piece.shape[0]
        copy = pltpu.make_async_copy(piece, keys.at[at : at + count], sems.at[index])
        copy.start()
        copies.append(copy)
        at += count
    for head in range(QPK):
        part = q_ref[:, head * HEAD : (head + 1) * HEAD].astype(jnp.float32)
        turned[:, head * L_DEV : (head + 1) * L_DEV] = jnp.transpose(part).astype(jnp.bfloat16)
    acc[...] = jnp.zeros_like(acc)
    top[...] = jnp.full_like(top, mask_floor)
    total[...] = jnp.zeros_like(total)
    mine = info_ref[2 * N_SEQ]
    for copy in copies:
        copy.wait()
    scale = math.log2(math.e) / math.sqrt(HEAD)

    def update(slot, masked):
        block = keys[slot]
        scores = jnp.dot(block[:, :HEAD], turned[...], preferred_element_type=jnp.float32) * scale
        if masked:
            shard = info_ref[slot]
            key_pos = shard * L_DEV + lax.broadcasted_iota(jnp.int32, (L_DEV, QPK * L_DEV), 0)
            column = lax.broadcasted_iota(jnp.int32, (L_DEV, QPK * L_DEV), 1)
            query_pos = mine * L_DEV + column % L_DEV
            allowed = (key_pos <= query_pos) & (key_pos >= low_ref[...])
            scores = jnp.where(allowed, scores, mask_floor)
        new_top = jnp.maximum(top[...], jnp.max(scores, axis=0, keepdims=True))
        weights = jnp.exp2(scores - new_top)
        if masked:
            weights = jnp.where(allowed, weights, 0.0)
        keep = jnp.exp2(top[...] - new_top)
        total[...] = total[...] * keep + jnp.sum(weights, axis=0, keepdims=True)
        acc[...] = acc[...] * keep + jnp.dot(
            block[:, HEAD:], weights.astype(jnp.bfloat16), preferred_element_type=jnp.float32
        )
        top[...] = new_top

    def visit(slot, carry):
        mode = info_ref[N_SEQ + slot]

        @pl.when(mode == 1)
        def _():
            update(slot, False)

        @pl.when(mode == 2)
        def _():
            update(slot, True)

        return carry

    lax.fori_loop(0, N_SEQ, visit, 0)
    mixed = acc[...] / total[...]
    for head in range(QPK):
        part = mixed[:, head * L_DEV : (head + 1) * L_DEV]
        out_ref[:, head * HEAD : (head + 1) * HEAD] = jnp.transpose(part).astype(jnp.bfloat16)


def attend(info, queries, lows, pieces):
    vmem = pl.BlockSpec(memory_space=pltpu.VMEM)
    return pl.pallas_call(
        attend_kernel,
        out_shape=jax.ShapeDtypeStruct((L_DEV, QPK * HEAD), jnp.bfloat16),
        in_specs=[pl.BlockSpec(memory_space=pltpu.SMEM), vmem, vmem]
        + [pl.BlockSpec(memory_space=pl.ANY)] * len(pieces),
        out_specs=vmem,
        scratch_shapes=[
            pltpu.VMEM((N_SEQ, L_DEV, 2 * HEAD), jnp.bfloat16),
            pltpu.VMEM((HEAD, QPK * L_DEV), jnp.bfloat16),
            pltpu.VMEM((HEAD, QPK * L_DEV), jnp.float32),
            pltpu.VMEM((1, QPK * L_DEV), jnp.float32),
            pltpu.VMEM((1, QPK * L_DEV), jnp.float32),
            pltpu.SemaphoreType.DMA((len(pieces),)),
        ],
        compiler_params=pltpu.CompilerParams(vmem_limit_bytes=24 * 1024 * 1024),
        name="attend",
    )(info, queries, lows, *pieces)


def shift(block, axis, step):
    size = lax.axis_size(axis)
    return lax.ppermute(block, axis, [(i, (i + step) % size) for i in range(size)])


def plane_gather(block, z, x, core):
    steps = (0, 4, 3, 5, 2, 6, 1, 7)
    column = jnp.stack([block] + [shift(block, "z", step) for step in steps[1:]])
    rows = (z - jnp.array(steps, jnp.int32)) % 8
    up = shift(column, "x", 1)
    down = shift(column, "x", 3)
    far_up = shift(up[:4], "x", 1)
    far_down = shift(down[4:], "x", 3)
    own = [column, up, down, far_up, far_down]
    swapped = [shift(piece, "core", 1) for piece in own]
    places = []
    for side in (core, 1 - core):
        for part, step in ((rows, 0), (rows, 1), (rows, 3), (rows[:4], 2), (rows[4:], 2)):
            places.append((part * 4 + (x - step) % 4) * 2 + side)
    return own + swapped, jnp.concatenate(places)


def rope_tables(positions):
    half = HEAD // 2
    rates = jnp.exp(jnp.arange(half, dtype=jnp.float32) * (-2.0 * math.log(rope_base) / HEAD))
    angles = positions.astype(jnp.float32)[:, None] * rates[None, :]
    return jnp.cos(angles), jnp.sin(angles)


def rotate(values, tables):
    cosine, sine = (table[:, None, :] for table in tables)
    half = HEAD // 2
    first, second = values[..., :half], values[..., half:]
    return jnp.concatenate([first * cosine - second * sine, second * cosine + first * sine], axis=-1)


def pick_matrix(offsets, count):
    valid = (offsets >= 0) & (offsets < count)
    columns = jnp.arange(POOL * POOL, dtype=jnp.int32)
    return ((offsets[:, None] == columns[None, :]) & valid[:, None]).astype(jnp.bfloat16), valid


def per_device(
    patches,
    fc_gain,
    fc_in,
    fc_in_bias,
    fc_out,
    fc_out_bias,
    proj_weight,
    text_embed,
    frame_start,
    frame_count,
    segment_ids,
    norm_gain,
    query_weight,
    query_bias,
    key_weight,
    value_weight,
    value_bias,
):
    section = lax.axis_index("section")
    z, x, core = (lax.axis_index(name).astype(jnp.int32) for name in SEQ)
    shard = (z * 4 + x) * 2 + core
    odd = section % 2 == 1

    main_in, left_in = fold_rows(jnp.concatenate([fc_in[0], jnp.transpose(fc_out[0])], axis=1))
    own_pack = jnp.concatenate([main_in, left_in], axis=1)
    own_small = jnp.concatenate([fc_gain[0], fc_in_bias[0], fc_out_bias[0]])
    pairs = [(0, 1), (1, 0), (2, 3), (3, 2)]
    other_pack = lax.ppermute(own_pack, "section", pairs)
    other_small = lax.ppermute(own_small, "section", pairs)
    packs = [jnp.where(odd, other_pack, own_pack), jnp.where(odd, own_pack, other_pack)]
    small = jnp.stack([jnp.where(odd, other_small, own_small), jnp.where(odd, own_small, other_small)])
    proj_main, proj_left = fold_rows(proj_weight)
    sent = jnp.concatenate(
        [packs[0][:, :LAYER_COLS], packs[1][:, :LAYER_COLS], proj_main]
        + [packs[0][:, LAYER_COLS:], packs[1][:, LAYER_COLS:], proj_left],
        axis=1,
    )
    full = lax.all_gather(sent, SEQ, axis=0, tiled=True)
    at = 2 * LAYER_COLS + HM
    fold = left_in.shape[1]
    left = jnp.concatenate(
        [unfold_rows(full[:, at + i * fold : at + (i + 1) * fold], LAYER_COLS) for i in range(2)], axis=1
    )
    proj_rest = unfold_rows(full[:, at + 2 * fold :], HM)

    gain = feature_order(small[:, :D])
    b_in = small[:, D : D + FF]
    b_out = feature_order(small[:, D + FF :])

    frame = jnp.pad(patches[0], ((0, 2 * HALF_ROWS - GRID * GRID), (0, 0)))
    half = jnp.where(odd, frame[:HALF_ROWS], frame[HALF_ROWS:])
    half = jnp.dot(half, order_matrix(), preferred_element_type=jnp.float32).astype(jnp.bfloat16)
    chunks = [half[:CHUNK_ROWS], half[CHUNK_ROWS:]]
    hop = [(1, 2), (0, 3)]
    passed = []
    for chunk in chunks:
        passed.append(lax.ppermute(encode(chunk, gain, b_in, b_out, left, full), "section", hop))
    ended = jnp.concatenate([encode(chunk, gain, b_in, b_out, left, full) for chunk in passed], axis=0)

    first_row = jnp.where(section == 3, POOL, 0)
    tokens = jnp.arange(POOL * POOL // 2, dtype=jnp.int32)
    patch = jnp.arange(HALF_ROWS, dtype=jnp.int32)
    patch_row, patch_col = patch // GRID, patch % GRID
    in_cell = (patch_row[None, :] // 2 == tokens[:, None] // POOL) & (
        patch_col[None, :] // 2 == tokens[:, None] % POOL
    )
    in_cell = in_cell & (patch_row + first_row < GRID)[None, :]
    tall = jnp.minimum(2, GRID - first_row - 2 * (tokens // POOL))
    wide = jnp.minimum(2, GRID - 2 * (tokens % POOL))
    area = (tall * wide).astype(jnp.float32)
    pooled = jnp.dot(in_cell.astype(jnp.bfloat16), ended, preferred_element_type=jnp.float32)
    pooled = (pooled / area[:, None]).astype(jnp.bfloat16)
    pooled = lax.all_gather(pooled, "section")
    pooled = jnp.concatenate([pooled[2], pooled[3]], axis=0)

    positions = shard * L_DEV + jnp.arange(L_DEV, dtype=jnp.int32)
    own_start, own_count = frame_start[shard], frame_count[shard]
    before = jnp.maximum(shard - 1, 0)
    prev_offsets = positions - frame_start[before]
    prev_valid = (shard > 0) & (prev_offsets >= 0) & (prev_offsets < frame_count[before])
    own_pick, own_valid = pick_matrix(positions - own_start, own_count)
    sent_pick, _ = pick_matrix(positions + L_DEV - own_start, own_count)
    picked = jnp.dot(
        jnp.concatenate([own_pick, sent_pick]), pooled, preferred_element_type=jnp.float32
    ).astype(jnp.bfloat16)
    arrived = lax.ppermute(picked[L_DEV:], SEQ, [(i, i + 1) for i in range(N_SEQ - 1)])
    vision = jnp.where(own_valid[:, None], picked[:L_DEV], arrived)
    projected = jnp.dot(
        vision[:, :MAIN], full[:, 2 * LAYER_COLS : at], preferred_element_type=jnp.float32
    ) + jnp.dot(vision[:, MAIN:], proj_rest, preferred_element_type=jnp.float32)
    inputs = jnp.where((own_valid | prev_valid)[:, None], projected.astype(jnp.bfloat16), text_embed)
    widened = inputs.astype(jnp.float32)
    normed = (
        widened * lax.rsqrt(jnp.mean(widened * widened, axis=1, keepdims=True) + rms_eps) * norm_gain
    ).astype(jnp.bfloat16)

    tables = rope_tables(positions)
    key_heads = jnp.dot(normed, key_weight, preferred_element_type=jnp.float32)
    key_heads = rotate(key_heads[:, None, :], tables)[:, 0].astype(jnp.bfloat16)
    values = (jnp.dot(normed, value_weight, preferred_element_type=jnp.float32) + value_bias).astype(jnp.bfloat16)
    block = jnp.concatenate([key_heads, jnp.transpose(values)], axis=1)
    pieces, places = plane_gather(block, z, x, core)
    queries = jnp.dot(normed, query_weight, preferred_element_type=jnp.float32) + query_bias
    queries = rotate(queries.reshape(L_DEV, QPK, HEAD), tables).astype(jnp.bfloat16).reshape(L_DEV, QPK * HEAD)

    starts = jnp.stack([jnp.sum((segment_ids < number).astype(jnp.int32)) for number in range(3)])
    mine = lax.dynamic_slice_in_dim(segment_ids, shard * L_DEV, L_DEV, 0)
    low = jnp.where(mine == 0, starts[0], jnp.where(mine == 1, starts[1], starts[2]))
    reached = (places <= shard) & ((places + 1) * L_DEV > low[0])
    whole = (places < shard) & (places * L_DEV >= low[L_DEV - 1])
    mode = jnp.where(reached, jnp.where(whole, 1, 2), 0)
    info = jnp.concatenate([places, mode, shard[None]]).astype(jnp.int32)
    return attend(info, queries, jnp.tile(low, QPK)[None, :], pieces)


def solution(mesh):
    axes = ("section",) + SEQ
    parts = Mesh(mesh.devices.reshape(4, 8, 4, 2), axes)
    return jax.shard_map(
        per_device,
        mesh=parts,
        in_specs=(
            P(SEQ, None, None),
            P("section", None),
            P("section", SEQ, None),
            P("section", None),
            P("section", None, SEQ),
            P("section", None),
            P(SEQ, None),
            P(SEQ, None),
            P(),
            P(),
            P(),
            P(),
            P(None, "section"),
            P("section"),
            P(None, "section"),
            P(None, "section"),
            P("section"),
        ),
        out_specs=P(SEQ, "section"),
        check_vma=False,
    )
```

```python
import math

import jax
import jax.numpy as jnp
from jax import lax
from jax.experimental import pallas as pl
from jax.experimental.pallas import tpu as pltpu
from jax.sharding import Mesh, PartitionSpec as P

GRID = 27
POOL = 14
D = 1152
FF = 2176
HM = 3584
HEAD = 128
QPK = 4
L_DEV = 128
N_SEQ = 64
MAIN = 1024
LEFT = 128
LAYER_COLS = 2 * FF
HALF_ROWS = POOL * GRID
CHUNK_ROWS = HALF_ROWS // 2
FF_CUTS = (0, 1024, 2176)
FOLD = 640
HM_CUTS = (0, 512, 1536, 2560, 3584)
AHEAD = 2
GROUP = 8

layer_eps = 1e-06
rms_eps = 1e-06
rope_base = 1000000.0
mask_floor = -1e30

SEQ = ("z", "x", "core")


def fold_rows(shard):
    width = shard.shape[1]
    piece = -(-width // (8 * 128)) * 128
    rest = jnp.pad(shard[16:], ((0, 0), (0, 8 * piece - width)))
    return shard[:16], rest.reshape(16, piece)


def feature_order(v):
    split = v.reshape(v.shape[:-1] + (N_SEQ, 18))
    main = split[..., :16].reshape(v.shape[:-1] + (MAIN,))
    left = split[..., 16:].reshape(v.shape[:-1] + (LEFT,))
    return jnp.concatenate([main, left], axis=-1)


def order_matrix():
    to = jnp.arange(D)
    low = (to // 16) * 18 + to % 16
    rest = to - MAIN
    high = (rest // 2) * 18 + 16 + rest % 2
    source = jnp.where(to < MAIN, low, high)
    return (jnp.arange(D)[:, None] == source[None, :]).astype(jnp.bfloat16)


def unfold(folded, place):
    out_row = lax.broadcasted_iota(jnp.int32, (128, 128), 0)
    in_row = lax.broadcasted_iota(jnp.int32, (128, 128), 1)
    source = (out_row % 16) // 2 * 16 + out_row % 2 * 8 + out_row // 16
    order = (in_row == source).astype(jnp.bfloat16)

    def one(group, carry):
        rows = folded[pl.ds(pl.multiple_of(group * 128, 128), 128), :]
        turned = jnp.dot(order, rows, preferred_element_type=jnp.float32).astype(jnp.bfloat16)
        for index in range(8):
            place(pl.multiple_of(group * 16, 16), index, turned[index * 16 : (index + 1) * 16])
        return carry

    lax.fori_loop(0, 8, one, 0)


def encoder_body(x_ref, small_ref, left_ref, out_ref, w_in, w_out, ready):
    gain_ref = small_ref.at[:, :D]
    bout_ref = small_ref.at[:, D : 2 * D]
    bin_ref = small_ref.at[:, 2 * D :]
    x = x_ref[...].astype(jnp.float32)
    last = (((1,), (1,)), ((), ()))
    for layer in range(2):
        base = layer * 8 * FOLD
        center = x - jnp.mean(x, axis=1, keepdims=True)
        spread = jnp.mean(center * center, axis=1, keepdims=True)
        normed = (center * lax.rsqrt(spread + layer_eps) * gain_ref[layer : layer + 1, :]).astype(jnp.bfloat16)
        acc_main = jnp.zeros((x.shape[0], MAIN), jnp.float32)
        acc_left = jnp.zeros((x.shape[0], LEFT), jnp.float32)
        for index, (lo, hi) in enumerate(zip(FF_CUTS[:-1], FF_CUTS[1:])):
            ready(layer, index)
            pre = jnp.dot(normed[:, :MAIN], w_in[layer, :, lo:hi], preferred_element_type=jnp.float32)
            pre = pre + jnp.dot(
                normed[:, MAIN:], left_ref[:, base + lo : base + hi], preferred_element_type=jnp.float32
            )
            hidden = jax.nn.gelu(pre + bin_ref[layer : layer + 1, lo:hi], approximate=True).astype(jnp.bfloat16)
            acc_main = acc_main + lax.dot_general(
                hidden, w_out[layer, :, lo:hi], last, preferred_element_type=jnp.float32
            )
            acc_left = acc_left + lax.dot_general(
                hidden, left_ref[:, base + FF + lo : base + FF + hi], last, preferred_element_type=jnp.float32
            )
        x = x + jnp.concatenate([acc_main, acc_left], axis=1) + bout_ref[layer : layer + 1, :]
        x = x.astype(jnp.bfloat16).astype(jnp.float32)
    out_ref[...] = x.astype(jnp.bfloat16)


def encoder_kernel(x_hbm, small_hbm, full_ref, *rest):
    if len(rest) == 10:
        out_ref, left_ref, w_in, w_out, sems, x_ref, small_ref, head_sems, folded, sem = rest
        fold_copy = pltpu.make_async_copy(full_ref.at[:, 2 * LAYER_COLS :], folded, sem)
        fold_copy.start()
    else:
        left_ref, out_ref, w_in, w_out, sems, x_ref, small_ref, head_sems = rest
        folded = None
    heads = (
        pltpu.make_async_copy(x_hbm, x_ref, head_sems.at[0]),
        pltpu.make_async_copy(small_hbm, small_ref, head_sems.at[1]),
    )
    for copy in heads:
        copy.start()
    cuts = list(zip(FF_CUTS[:-1], FF_CUTS[1:]))
    copies = []
    for layer in range(2):
        base = layer * LAYER_COLS
        for index, (lo, hi) in enumerate(cuts):
            copies.append(
                [
                    pltpu.make_async_copy(
                        full_ref.at[:, base + shift + lo : base + shift + hi],
                        buf.at[layer, :, lo:hi],
                        sems.at[layer, index, kind],
                    )
                    for kind, (buf, shift) in enumerate(((w_in, 0), (w_out, FF)))
                ]
            )
    for pair in copies[:AHEAD]:
        for copy in pair:
            copy.start()
    if folded is not None:
        fold_copy.wait()

        def place(row, index, block):
            for layer in range(2):
                at = (layer * 8 + index) * FOLD
                left_ref[pl.ds(row, 16), at : at + FOLD] = block[:, layer * FOLD : (layer + 1) * FOLD]

        unfold(folded, place)

    for copy in heads:
        copy.wait()

    def ready(layer, index):
        step = layer * len(cuts) + index
        for copy in copies[step]:
            copy.wait()
        if step + AHEAD < len(copies):
            for copy in copies[step + AHEAD]:
                copy.start()

    encoder_body(x_ref, small_ref, left_ref, out_ref, w_in, w_out, ready)


def encode(x, small, full, left=None):
    vmem = pl.BlockSpec(memory_space=pltpu.VMEM)
    out_shape = [jax.ShapeDtypeStruct(x.shape, jnp.bfloat16)]
    scratch = [
        pltpu.VMEM((2, MAIN, FF), jnp.bfloat16),
        pltpu.VMEM((2, MAIN, FF), jnp.bfloat16),
        pltpu.SemaphoreType.DMA((2, len(FF_CUTS) - 1, 2)),
    ]
    scratch += [
        pltpu.VMEM(x.shape, jnp.bfloat16),
        pltpu.VMEM(small.shape, jnp.float32),
        pltpu.SemaphoreType.DMA((2,)),
    ]
    given = ()
    if left is None:
        out_shape.append(jax.ShapeDtypeStruct((LEFT, 2 * 8 * FOLD), jnp.bfloat16))
        scratch += [pltpu.VMEM((MAIN, 2 * FOLD), jnp.bfloat16), pltpu.SemaphoreType.DMA]
    else:
        given = (left,)
    return pl.pallas_call(
        encoder_kernel,
        out_shape=out_shape,
        in_specs=[pl.BlockSpec(memory_space=pl.ANY)] * 3 + [vmem] * len(given),
        out_specs=[vmem] * len(out_shape),
        scratch_shapes=scratch,
        compiler_params=pltpu.CompilerParams(vmem_limit_bytes=45 * 1024 * 1024),
        name="encoder_pair",
    )(x, small, full, *given)


def pick_kernel(want_ref, ids_ref, tokens_ref, out_ref):
    pick = (want_ref[...] == ids_ref[...]).astype(jnp.bfloat16)
    out_ref[...] = jnp.dot(pick, tokens_ref[...], preferred_element_type=jnp.float32).astype(jnp.bfloat16)


def pick_rows(want, ids, tokens):
    vmem = pl.BlockSpec(memory_space=pltpu.VMEM)
    return pl.pallas_call(
        pick_kernel,
        out_shape=jax.ShapeDtypeStruct((want.shape[0], D), jnp.bfloat16),
        in_specs=[vmem] * 3,
        out_specs=vmem,
        compiler_params=pltpu.CompilerParams(vmem_limit_bytes=16 * 1024 * 1024),
        name="pick_rows",
    )(want, ids, tokens)


def project_kernel(vision_ref, text_ref, use_ref, gain_ref, proj_ref, out_ref, weights, folded, rest, sems, sem):
    fold_copy = pltpu.make_async_copy(proj_ref.at[:, HM:], folded, sem)
    fold_copy.start()
    cuts = list(zip(HM_CUTS[:-1], HM_CUTS[1:]))
    copies = [
        pltpu.make_async_copy(proj_ref.at[:, lo:hi], weights.at[:, lo:hi], sems.at[index])
        for index, (lo, hi) in enumerate(cuts)
    ]
    for copy in copies:
        copy.start()
    fold_copy.wait()
    width = folded.shape[1]

    def place(row, index, block):
        rest[pl.ds(row, 16), index * width : (index + 1) * width] = block

    unfold(folded, place)
    use = use_ref[...] > 0
    vision = vision_ref[...]
    squares = jnp.zeros((L_DEV, 1), jnp.float32)
    for copy, (lo, hi) in zip(copies, cuts):
        copy.wait()
        projected = jnp.dot(vision[:, :MAIN], weights[:, lo:hi], preferred_element_type=jnp.float32)
        projected = projected + jnp.dot(vision[:, MAIN:], rest[:, lo:hi], preferred_element_type=jnp.float32)
        projected = projected.astype(jnp.bfloat16).astype(jnp.float32)
        inputs = jnp.where(use, projected, text_ref[:, lo:hi].astype(jnp.float32))
        squares = squares + jnp.sum(inputs * inputs, axis=1, keepdims=True)
        out_ref[:, lo:hi] = inputs.astype(jnp.bfloat16)
    scale = lax.rsqrt(squares / HM + rms_eps)
    for lo, hi in cuts:
        inputs = out_ref[:, lo:hi].astype(jnp.float32)
        out_ref[:, lo:hi] = (inputs * scale * gain_ref[:, lo:hi]).astype(jnp.bfloat16)


def project(vision, text, use_vision, gain, proj_full):
    vmem = pl.BlockSpec(memory_space=pltpu.VMEM)
    width = proj_full.shape[1] - HM
    return pl.pallas_call(
        project_kernel,
        out_shape=jax.ShapeDtypeStruct((L_DEV, HM), jnp.bfloat16),
        in_specs=[vmem] * 4 + [pl.BlockSpec(memory_space=pl.ANY)],
        out_specs=vmem,
        scratch_shapes=[
            pltpu.VMEM((MAIN, HM), jnp.bfloat16),
            pltpu.VMEM((MAIN, width), jnp.bfloat16),
            pltpu.VMEM((LEFT, 8 * width), jnp.bfloat16),
            pltpu.SemaphoreType.DMA((len(HM_CUTS) - 1,)),
            pltpu.SemaphoreType.DMA,
        ],
        compiler_params=pltpu.CompilerParams(vmem_limit_bytes=56 * 1024 * 1024),
        name="project",
    )(vision, text, use_vision, gain, proj_full)


def attend_kernel(info_ref, q_ref, low_ref, *rest):
    pieces, (out_ref, keys, turned, acc, top, total, sems) = rest[:10], rest[10:]
    copies, at = [], 0
    for index, piece in enumerate(pieces):
        count = piece.shape[0]
        copy = pltpu.make_async_copy(piece, keys.at[at : at + count], sems.at[index])
        copy.start()
        copies.append(copy)
        at += count
    for head in range(QPK):
        part = q_ref[:, head * HEAD : (head + 1) * HEAD].astype(jnp.float32)
        turned[:, head * L_DEV : (head + 1) * L_DEV] = jnp.transpose(part).astype(jnp.bfloat16)
    acc[...] = jnp.zeros_like(acc)
    top[...] = jnp.full_like(top, mask_floor)
    total[...] = jnp.zeros_like(total)
    first, whole, mine = (info_ref[N_SEQ + index] for index in range(3))
    for copy in copies:
        copy.wait()
    scale = math.log2(math.e) / math.sqrt(HEAD)

    def update(start, masked):
        blocks = [keys[info_ref[jnp.minimum(start + index, mine)]] for index in range(GROUP)]
        scores = jnp.concatenate(
            [jnp.dot(block[:, :HEAD], turned[...], preferred_element_type=jnp.float32) for block in blocks]
        )
        scores = scores * scale
        if masked:
            key_pos = start * L_DEV + lax.broadcasted_iota(jnp.int32, scores.shape, 0)
            query_pos = mine * L_DEV + lax.broadcasted_iota(jnp.int32, scores.shape, 1) % L_DEV
            allowed = (key_pos <= query_pos) & (key_pos >= low_ref[...])
            scores = jnp.where(allowed, scores, mask_floor)
        new_top = jnp.maximum(top[...], jnp.max(scores, axis=0, keepdims=True))
        weights = jnp.exp2(scores - new_top)
        if masked:
            weights = jnp.where(allowed, weights, 0.0)
        keep = jnp.exp2(top[...] - new_top)
        total[...] = total[...] * keep + jnp.sum(weights, axis=0, keepdims=True)
        acc[...] = acc[...] * keep + jnp.dot(
            jnp.concatenate([block[:, HEAD:] for block in blocks], axis=1),
            weights.astype(jnp.bfloat16),
            preferred_element_type=jnp.float32,
        )
        top[...] = new_top

    def visit(group, carry):
        start = first + group * GROUP
        plain = (start >= whole) & (start + GROUP <= mine)

        @pl.when(plain)
        def _():
            update(start, False)

        @pl.when(jnp.logical_not(plain))
        def _():
            update(start, True)

        return carry

    lax.fori_loop(0, (mine - first) // GROUP + 1, visit, 0)
    mixed = acc[...] / total[...]
    for head in range(QPK):
        part = mixed[:, head * L_DEV : (head + 1) * L_DEV]
        out_ref[:, head * HEAD : (head + 1) * HEAD] = jnp.transpose(part).astype(jnp.bfloat16)


def attend(info, queries, lows, pieces):
    vmem = pl.BlockSpec(memory_space=pltpu.VMEM)
    return pl.pallas_call(
        attend_kernel,
        out_shape=jax.ShapeDtypeStruct((L_DEV, QPK * HEAD), jnp.bfloat16),
        in_specs=[pl.BlockSpec(memory_space=pltpu.SMEM), vmem, vmem]
        + [pl.BlockSpec(memory_space=pl.ANY)] * len(pieces),
        out_specs=vmem,
        scratch_shapes=[
            pltpu.VMEM((N_SEQ, L_DEV, 2 * HEAD), jnp.bfloat16),
            pltpu.VMEM((HEAD, QPK * L_DEV), jnp.bfloat16),
            pltpu.VMEM((HEAD, QPK * L_DEV), jnp.float32),
            pltpu.VMEM((1, QPK * L_DEV), jnp.float32),
            pltpu.VMEM((1, QPK * L_DEV), jnp.float32),
            pltpu.SemaphoreType.DMA((len(pieces),)),
        ],
        compiler_params=pltpu.CompilerParams(vmem_limit_bytes=24 * 1024 * 1024),
        name="attend",
    )(info, queries, lows, *pieces)


def shift(block, axis, step):
    size = lax.axis_size(axis)
    return lax.ppermute(block, axis, [(i, (i + step) % size) for i in range(size)])


Z_STEPS = (0, 4, 3, 5, 2, 6, 1, 7)


def plane_gather(block):
    column = jnp.stack([block] + [shift(block, "z", step) for step in Z_STEPS[1:]])
    up = shift(column, "x", 1)
    down = shift(column, "x", 3)
    far_up = shift(up[:4], "x", 1)
    far_down = shift(down[4:], "x", 3)
    own = [column, up, down, far_up, far_down]
    return own + [shift(piece, "core", 1) for piece in own]


def plane_places(z, x, core):
    rows = (z - jnp.array(Z_STEPS, jnp.int32)) % 8
    places = []
    for side in (core, 1 - core):
        for part, step in ((rows, 0), (rows, 1), (rows, 3), (rows[:4], 2), (rows[4:], 2)):
            places.append((part * 4 + (x - step) % 4) * 2 + side)
    return jnp.concatenate(places)


def rope_tables(positions):
    half = HEAD // 2
    rates = jnp.exp(jnp.arange(half, dtype=jnp.float32) * (-2.0 * math.log(rope_base) / HEAD))
    angles = positions.astype(jnp.float32)[:, None] * rates[None, :]
    return jnp.cos(angles), jnp.sin(angles)


def rotate(values, tables):
    cosine, sine = (table[:, None, :] for table in tables)
    half = HEAD // 2
    first, second = values[..., :half], values[..., half:]
    return jnp.concatenate([first * cosine - second * sine, second * cosine + first * sine], axis=-1)


def per_device(
    patches,
    fc_gain,
    fc_in,
    fc_in_bias,
    fc_out,
    fc_out_bias,
    proj_weight,
    text_embed,
    frame_start,
    frame_count,
    segment_ids,
    norm_gain,
    query_weight,
    query_bias,
    key_weight,
    value_weight,
    value_bias,
):
    section = lax.axis_index("section")
    z, x, core = (lax.axis_index(name).astype(jnp.int32) for name in SEQ)
    shard = (z * 4 + x) * 2 + core
    odd = section % 2 == 1

    main_in, left_in = fold_rows(jnp.concatenate([fc_in[0], jnp.transpose(fc_out[0])], axis=1))
    own_pack = jnp.concatenate([main_in, left_in], axis=1)
    own_small = jnp.concatenate([fc_gain[0], fc_in_bias[0], fc_out_bias[0]])
    pairs = [(0, 1), (1, 0), (2, 3), (3, 2)]
    other_pack = lax.ppermute(own_pack, "section", pairs)
    other_small = lax.ppermute(own_small, "section", pairs)
    packs = [jnp.where(odd, other_pack, own_pack), jnp.where(odd, own_pack, other_pack)]
    small = jnp.stack([jnp.where(odd, other_small, own_small), jnp.where(odd, own_small, other_small)])
    sent = jnp.concatenate(
        [pack[:, :LAYER_COLS] for pack in packs] + [pack[:, LAYER_COLS:] for pack in packs], axis=1
    )
    full = lax.all_gather(sent, SEQ, axis=0, tiled=True)
    proj_full = lax.all_gather(jnp.concatenate(fold_rows(proj_weight), axis=1), SEQ, axis=0, tiled=True)

    small = jnp.concatenate(
        [feature_order(small[:, :D]), feature_order(small[:, D + FF :]), small[:, D : D + FF]], axis=1
    )

    frame = jnp.pad(patches[0], ((0, 2 * HALF_ROWS - GRID * GRID), (0, 0)))
    half = jnp.where(odd, frame[:HALF_ROWS], frame[HALF_ROWS:])
    half = jnp.dot(half, order_matrix(), preferred_element_type=jnp.float32).astype(jnp.bfloat16)
    chunks = [half[:CHUNK_ROWS], half[CHUNK_ROWS:]]

    first_row = jnp.where(section == 3, POOL, 0)
    tokens = jnp.arange(POOL * POOL // 2, dtype=jnp.int32)
    patch = jnp.arange(HALF_ROWS, dtype=jnp.int32)
    patch_row, patch_col = patch // GRID, patch % GRID
    in_cell = (patch_row[None, :] // 2 == tokens[:, None] // POOL) & (
        patch_col[None, :] // 2 == tokens[:, None] % POOL
    )
    in_cell = (in_cell & (patch_row + first_row < GRID)[None, :]).astype(jnp.bfloat16)
    tall = jnp.minimum(2, GRID - first_row - 2 * (tokens // POOL))
    wide = jnp.minimum(2, GRID - 2 * (tokens % POOL))
    area = (tall * wide).astype(jnp.float32)[:, None]

    positions = shard * L_DEV + jnp.arange(L_DEV, dtype=jnp.int32)
    own_start, own_count = frame_start[shard], frame_count[shard]
    before = jnp.maximum(shard - 1, 0)
    prev_offsets = positions - frame_start[before]
    prev_valid = (shard > 0) & (prev_offsets >= 0) & (prev_offsets < frame_count[before])
    own_valid = (positions >= own_start) & (positions < own_start + own_count)
    use_vision = (own_valid | prev_valid).astype(jnp.float32)[:, None]
    use_own = own_valid.astype(jnp.float32)[:, None]
    want = jnp.concatenate([positions, positions + L_DEV]) - own_start
    want = jnp.where((want >= 0) & (want < own_count), want, -2)[:, None]
    held = jnp.arange(4 * POOL * POOL // 2, dtype=jnp.int32) - POOL * POOL
    ids = jnp.where(held >= 0, held, -1)[None, :]

    starts = jnp.stack([jnp.sum((segment_ids < number).astype(jnp.int32)) for number in range(3)])
    mine = lax.dynamic_slice_in_dim(segment_ids, shard * L_DEV, L_DEV, 0)
    low = jnp.where(mine == 0, starts[0], jnp.where(mine == 1, starts[1], starts[2]))
    places = plane_places(z, x, core)
    slots = jnp.zeros((N_SEQ,), jnp.int32).at[places].set(jnp.arange(N_SEQ, dtype=jnp.int32))
    edges = jnp.stack([low[0] // L_DEV, (low[L_DEV - 1] + L_DEV - 1) // L_DEV, shard])
    info = jnp.concatenate([slots, edges]).astype(jnp.int32)
    lows = jnp.tile(low, QPK)[None, :]
    tables = rope_tables(positions)

    full, small, chunks, in_cell, area, use_vision, use_own, want, ids, info, lows, tables = (
        lax.optimization_barrier(
            (full, small, chunks, in_cell, area, use_vision, use_own, want, ids, info, lows, tables)
        )
    )
    hop = [(1, 2), (0, 3)]
    ended, left = encode(chunks[0], small, full)
    passed = [lax.ppermute(ended, "section", hop)]
    (ended,) = encode(chunks[1], small, full, left)
    passed.append(lax.ppermute(ended, "section", hop))
    ended = jnp.concatenate([encode(chunk, small, full, left)[0] for chunk in passed], axis=0)
    pooled = jnp.dot(in_cell, ended, preferred_element_type=jnp.float32)
    pooled = lax.all_gather((pooled / area).astype(jnp.bfloat16), "section", tiled=True)
    picked = pick_rows(want, ids, pooled)
    arrived = lax.ppermute(picked[L_DEV:], SEQ, [(i, i + 1) for i in range(N_SEQ - 1)])
    vision = jnp.where(use_own > 0, picked[:L_DEV], arrived)
    vision, proj_full = lax.optimization_barrier((vision, proj_full))
    normed = project(vision, text_embed, use_vision, norm_gain[None, :], proj_full)

    key_heads = jnp.dot(normed, key_weight, preferred_element_type=jnp.float32)
    key_heads = rotate(key_heads[:, None, :], tables)[:, 0].astype(jnp.bfloat16)
    values = (jnp.dot(normed, value_weight, preferred_element_type=jnp.float32) + value_bias).astype(jnp.bfloat16)
    block = jnp.concatenate([key_heads, jnp.transpose(values)], axis=1)
    pieces = plane_gather(block)
    queries = jnp.dot(normed, query_weight, preferred_element_type=jnp.float32) + query_bias
    queries = rotate(queries.reshape(L_DEV, QPK, HEAD), tables).astype(jnp.bfloat16).reshape(L_DEV, QPK * HEAD)
    return attend(info, queries, lows, pieces)


def solution(mesh):
    axes = ("section",) + SEQ
    parts = Mesh(mesh.devices.reshape(4, 8, 4, 2), axes)
    return jax.shard_map(
        per_device,
        mesh=parts,
        in_specs=(
            P(SEQ, None, None),
            P("section", None),
            P("section", SEQ, None),
            P("section", None),
            P("section", None, SEQ),
            P("section", None),
            P(SEQ, None),
            P(SEQ, None),
            P(),
            P(),
            P(),
            P(),
            P(None, "section"),
            P("section"),
            P(None, "section"),
            P(None, "section"),
            P("section"),
        ),
        out_specs=P(SEQ, "section"),
        check_vma=False,
    )
```

```python
import functools
import math

import jax
import jax.numpy as jnp
from jax import lax
from jax.experimental import pallas as pl
from jax.experimental.pallas import tpu as pltpu
from jax.sharding import Mesh, PartitionSpec as P

GRID = 27
POOL = 14
D = 1152
FF = 2176
HM = 3584
HEAD = 128
QPK = 4
L_DEV = 128
N_SEQ = 64
MAIN = 1024
LEFT = 128
LAYER_COLS = 2 * FF
HALF_ROWS = POOL * GRID
CHUNK_ROWS = HALF_ROWS // 2
FF_CUTS = (0, 1024, 2176)
FOLD = 640
HM_CUTS = (0, 512, 1536, 2560, 3584)
AHEAD = 2
GROUP = 4

layer_eps = 1e-06
rms_eps = 1e-06
rope_base = 1000000.0
mask_floor = -1e30

SEQ = ("z", "x", "core")


def fold_rows(shard):
    width = shard.shape[1]
    piece = -(-width // (8 * 128)) * 128
    rest = jnp.pad(shard[16:], ((0, 0), (0, 8 * piece - width)))
    return shard[:16], rest.reshape(16, piece)


def feature_order(v):
    split = v.reshape(v.shape[:-1] + (N_SEQ, 18))
    main = split[..., :16].reshape(v.shape[:-1] + (MAIN,))
    left = split[..., 16:].reshape(v.shape[:-1] + (LEFT,))
    return jnp.concatenate([main, left], axis=-1)


def order_matrix():
    to = jnp.arange(D)
    low = (to // 16) * 18 + to % 16
    rest = to - MAIN
    high = (rest // 2) * 18 + 16 + rest % 2
    source = jnp.where(to < MAIN, low, high)
    return (jnp.arange(D)[:, None] == source[None, :]).astype(jnp.bfloat16)


def unfold(folded, place):
    out_row = lax.broadcasted_iota(jnp.int32, (128, 128), 0)
    in_row = lax.broadcasted_iota(jnp.int32, (128, 128), 1)
    source = (out_row % 16) // 2 * 16 + out_row % 2 * 8 + out_row // 16
    order = (in_row == source).astype(jnp.bfloat16)

    def one(group, carry):
        rows = folded[pl.ds(pl.multiple_of(group * 128, 128), 128), :]
        turned = jnp.dot(order, rows, preferred_element_type=jnp.float32).astype(jnp.bfloat16)
        for index in range(8):
            place(pl.multiple_of(group * 16, 16), index, turned[index * 16 : (index + 1) * 16])
        return carry

    lax.fori_loop(0, 8, one, 0)


def encoder_body(x_ref, small_ref, left_ref, out_ref, w_in, w_out, ready):
    gain_ref = small_ref.at[:, :D]
    bout_ref = small_ref.at[:, D : 2 * D]
    bin_ref = small_ref.at[:, 2 * D :]
    last = (((1,), (1,)), ((), ()))

    def one_layer(layer, carry):
        x = x_ref[...].astype(jnp.float32)
        base = pl.multiple_of(layer * 8 * FOLD, 128)
        center = x - jnp.mean(x, axis=1, keepdims=True)
        spread = jnp.mean(center * center, axis=1, keepdims=True)
        normed = (center * lax.rsqrt(spread + layer_eps) * gain_ref[pl.ds(layer, 1), :]).astype(jnp.bfloat16)
        acc_main = jnp.zeros((x.shape[0], MAIN), jnp.float32)
        acc_left = jnp.zeros((x.shape[0], LEFT), jnp.float32)
        for index, (lo, hi) in enumerate(zip(FF_CUTS[:-1], FF_CUTS[1:])):
            ready(layer, index)
            pre = jnp.dot(normed[:, :MAIN], w_in[layer, :, lo:hi], preferred_element_type=jnp.float32)
            pre = pre + jnp.dot(
                normed[:, MAIN:], left_ref[:, pl.ds(base + lo, hi - lo)], preferred_element_type=jnp.float32
            )
            hidden = jax.nn.gelu(pre + bin_ref[pl.ds(layer, 1), lo:hi], approximate=True).astype(jnp.bfloat16)
            acc_main = acc_main + lax.dot_general(
                hidden, w_out[layer, :, lo:hi], last, preferred_element_type=jnp.float32
            )
            acc_left = acc_left + lax.dot_general(
                hidden, left_ref[:, pl.ds(base + FF + lo, hi - lo)], last, preferred_element_type=jnp.float32
            )
        x = x + jnp.concatenate([acc_main, acc_left], axis=1) + bout_ref[pl.ds(layer, 1), :]
        x_ref[...] = x.astype(jnp.bfloat16)
        return carry

    lax.fori_loop(0, 2, one_layer, 0)
    out_ref[...] = x_ref[...]


def encoder_kernel(x_hbm, small_hbm, full_ref, *rest):
    if len(rest) == 10:
        out_ref, left_ref, w_in, w_out, sems, x_ref, small_ref, head_sems, folded, sem = rest
        fold_copy = pltpu.make_async_copy(full_ref.at[:, 2 * LAYER_COLS :], folded, sem)
        fold_copy.start()
    else:
        left_ref, out_ref, w_in, w_out, sems, x_ref, small_ref, head_sems = rest
        folded = None
    heads = (
        pltpu.make_async_copy(x_hbm, x_ref, head_sems.at[0]),
        pltpu.make_async_copy(small_hbm, small_ref, head_sems.at[1]),
    )
    for copy in heads:
        copy.start()
    cuts = list(zip(FF_CUTS[:-1], FF_CUTS[1:]))
    copies = []
    for layer in range(2):
        base = layer * LAYER_COLS
        for index, (lo, hi) in enumerate(cuts):
            copies.append(
                [
                    pltpu.make_async_copy(
                        full_ref.at[:, base + shift + lo : base + shift + hi],
                        buf.at[layer, :, lo:hi],
                        sems.at[layer, index, kind],
                    )
                    for kind, (buf, shift) in enumerate(((w_in, 0), (w_out, FF)))
                ]
            )
    for pair in copies[:AHEAD]:
        for copy in pair:
            copy.start()
    if folded is not None:
        fold_copy.wait()

        def place(row, index, block):
            for layer in range(2):
                at = (layer * 8 + index) * FOLD
                left_ref[pl.ds(row, 16), at : at + FOLD] = block[:, layer * FOLD : (layer + 1) * FOLD]

        unfold(folded, place)

    for copy in heads:
        copy.wait()

    def ready(layer, index):
        @pl.when(layer == 0)
        def _():
            for copy in copies[index]:
                copy.wait()
            for copy in copies[index + AHEAD]:
                copy.start()

        @pl.when(layer == 1)
        def _():
            for copy in copies[index + AHEAD]:
                copy.wait()

    encoder_body(x_ref, small_ref, left_ref, out_ref, w_in, w_out, ready)


def encode(x, small, full, left=None):
    vmem = pl.BlockSpec(memory_space=pltpu.VMEM)
    out_shape = [jax.ShapeDtypeStruct(x.shape, jnp.bfloat16)]
    scratch = [
        pltpu.VMEM((2, MAIN, FF), jnp.bfloat16),
        pltpu.VMEM((2, MAIN, FF), jnp.bfloat16),
        pltpu.SemaphoreType.DMA((2, len(FF_CUTS) - 1, 2)),
    ]
    scratch += [
        pltpu.VMEM(x.shape, jnp.bfloat16),
        pltpu.VMEM(small.shape, jnp.float32),
        pltpu.SemaphoreType.DMA((2,)),
    ]
    given = ()
    if left is None:
        out_shape.append(jax.ShapeDtypeStruct((LEFT, 2 * 8 * FOLD), jnp.bfloat16))
        scratch += [pltpu.VMEM((MAIN, 2 * FOLD), jnp.bfloat16), pltpu.SemaphoreType.DMA]
    else:
        given = (left,)
    return pl.pallas_call(
        encoder_kernel,
        out_shape=out_shape,
        in_specs=[pl.BlockSpec(memory_space=pl.ANY)] * 3 + [vmem] * len(given),
        out_specs=[vmem] * len(out_shape),
        scratch_shapes=scratch,
        compiler_params=pltpu.CompilerParams(vmem_limit_bytes=45 * 1024 * 1024),
        name="encoder_pair",
    )(x, small, full, *given)


def pick_kernel(want_ref, ids_ref, tokens_ref, out_ref):
    pick = (want_ref[...] == ids_ref[...]).astype(jnp.bfloat16)
    out_ref[...] = jnp.dot(pick, tokens_ref[...], preferred_element_type=jnp.float32).astype(jnp.bfloat16)


def pick_rows(want, ids, tokens):
    vmem = pl.BlockSpec(memory_space=pltpu.VMEM)
    return pl.pallas_call(
        pick_kernel,
        out_shape=jax.ShapeDtypeStruct((want.shape[0], D), jnp.bfloat16),
        in_specs=[vmem] * 3,
        out_specs=vmem,
        compiler_params=pltpu.CompilerParams(vmem_limit_bytes=16 * 1024 * 1024),
        name="pick_rows",
    )(want, ids, tokens)


def project_kernel(vision_ref, text_hbm, use_ref, gain_ref, proj_ref, out_ref, weights, folded, rest, text_ref, sems, sem, text_sem):
    text_copy = pltpu.make_async_copy(text_hbm, text_ref, text_sem)
    text_copy.start()
    fold_copy = pltpu.make_async_copy(proj_ref.at[:, HM:], folded, sem)
    fold_copy.start()
    cuts = list(zip(HM_CUTS[:-1], HM_CUTS[1:]))
    copies = [
        pltpu.make_async_copy(proj_ref.at[:, lo:hi], weights.at[:, lo:hi], sems.at[index])
        for index, (lo, hi) in enumerate(cuts)
    ]
    for copy in copies:
        copy.start()
    fold_copy.wait()
    width = folded.shape[1]

    def place(row, index, block):
        rest[pl.ds(row, 16), index * width : (index + 1) * width] = block

    unfold(folded, place)
    text_copy.wait()
    use = use_ref[...] > 0
    vision = vision_ref[...]
    squares = jnp.zeros((L_DEV, 1), jnp.float32)
    for copy, (lo, hi) in zip(copies, cuts):
        copy.wait()
        projected = jnp.dot(vision[:, :MAIN], weights[:, lo:hi], preferred_element_type=jnp.float32)
        projected = projected + jnp.dot(vision[:, MAIN:], rest[:, lo:hi], preferred_element_type=jnp.float32)
        projected = projected.astype(jnp.bfloat16).astype(jnp.float32)
        inputs = jnp.where(use, projected, text_ref[:, lo:hi].astype(jnp.float32))
        squares = squares + jnp.sum(inputs * inputs, axis=1, keepdims=True)
        out_ref[:, lo:hi] = inputs.astype(jnp.bfloat16)
    scale = lax.rsqrt(squares / HM + rms_eps)
    for lo, hi in cuts:
        inputs = out_ref[:, lo:hi].astype(jnp.float32)
        out_ref[:, lo:hi] = (inputs * scale * gain_ref[:, lo:hi]).astype(jnp.bfloat16)


def project(vision, text, use_vision, gain, proj_full):
    vmem = pl.BlockSpec(memory_space=pltpu.VMEM)
    hbm = pl.BlockSpec(memory_space=pl.ANY)
    width = proj_full.shape[1] - HM
    return pl.pallas_call(
        project_kernel,
        out_shape=jax.ShapeDtypeStruct((L_DEV, HM), jnp.bfloat16),
        in_specs=[vmem, hbm, vmem, vmem, hbm],
        out_specs=vmem,
        scratch_shapes=[
            pltpu.VMEM((MAIN, HM), jnp.bfloat16),
            pltpu.VMEM((MAIN, width), jnp.bfloat16),
            pltpu.VMEM((LEFT, 8 * width), jnp.bfloat16),
            pltpu.VMEM((L_DEV, HM), jnp.bfloat16),
            pltpu.SemaphoreType.DMA((len(HM_CUTS) - 1,)),
            pltpu.SemaphoreType.DMA,
            pltpu.SemaphoreType.DMA,
        ],
        compiler_params=pltpu.CompilerParams(vmem_limit_bytes=56 * 1024 * 1024),
        name="project",
    )(vision, text, use_vision, gain, proj_full)


def query_kernel(normed_ref, bias_ref, cos_ref, sin_ref, weight_hbm, out_ref, weight, sem):
    copy = pltpu.make_async_copy(weight_hbm, weight, sem)
    copy.start()
    copy.wait()
    queries = jnp.dot(normed_ref[...], weight[...], preferred_element_type=jnp.float32) + bias_ref[...]
    for head in range(QPK):
        part = queries[:, head * HEAD : (head + 1) * HEAD]
        part = part * cos_ref[...] + pltpu.roll(part, HEAD // 2, 1) * sin_ref[...]
        part = jnp.transpose(part.astype(jnp.bfloat16).astype(jnp.float32))
        out_ref[:, head * L_DEV : (head + 1) * L_DEV] = part.astype(jnp.bfloat16)


def turned_queries(normed, bias, tables, weight):
    vmem = pl.BlockSpec(memory_space=pltpu.VMEM)
    cosine, sine = tables
    return pl.pallas_call(
        query_kernel,
        out_shape=jax.ShapeDtypeStruct((HEAD, QPK * L_DEV), jnp.bfloat16),
        in_specs=[vmem] * 4 + [pl.BlockSpec(memory_space=pl.ANY)],
        out_specs=vmem,
        scratch_shapes=[pltpu.VMEM(weight.shape, jnp.bfloat16), pltpu.SemaphoreType.DMA],
        compiler_params=pltpu.CompilerParams(vmem_limit_bytes=24 * 1024 * 1024),
        name="turned_queries",
    )(
        normed,
        bias[None, :],
        jnp.concatenate([cosine, cosine], axis=1),
        jnp.concatenate([-sine, sine], axis=1),
        weight,
    )


def attend_stage(last, info_ref, turned, low_ref, acc_in, top_in, total_in, *rest):
    pieces, rest = rest[: -6 if last else -5], rest[-6 if last else -5 :]
    if last:
        out_ref, acc, top, total, keys, sems = rest
    else:
        acc, top, total, keys, sems = rest
    copies, at = [], 0
    for index, piece in enumerate(pieces):
        copy = pltpu.make_async_copy(piece, keys.at[at : at + piece.shape[0]], sems.at[index])
        copy.start()
        copies.append(copy)
        at += piece.shape[0]
    acc[...] = acc_in[...]
    top[...] = top_in[...]
    total[...] = total_in[...]
    first, whole, mine = (info_ref[at + index] for index in range(3))
    for copy in copies:
        copy.wait()
    scale = math.log2(math.e) / math.sqrt(HEAD)

    def update(start, masked):
        blocks = [keys[start + index] for index in range(GROUP)]
        parts = []
        for index, block in enumerate(blocks):
            scores = jnp.dot(block[:, :HEAD], turned[...], preferred_element_type=jnp.float32) * scale
            if masked:
                key_pos = info_ref[start + index] * L_DEV + lax.broadcasted_iota(jnp.int32, scores.shape, 0)
                query_pos = mine * L_DEV + lax.broadcasted_iota(jnp.int32, scores.shape, 1) % L_DEV
                scores = jnp.where((key_pos <= query_pos) & (key_pos >= low_ref[...]), scores, mask_floor)
            parts.append(scores)
        scores = jnp.concatenate(parts)
        new_top = jnp.maximum(top[...], jnp.max(scores, axis=0, keepdims=True))
        weights = jnp.exp2(scores - new_top)
        keep = jnp.exp2(top[...] - new_top)
        total[...] = total[...] * keep + jnp.sum(weights, axis=0, keepdims=True)
        acc[...] = acc[...] * keep + jnp.dot(
            jnp.concatenate([block[:, HEAD:] for block in blocks], axis=1),
            weights.astype(jnp.bfloat16),
            preferred_element_type=jnp.float32,
        )
        top[...] = new_top

    def visit(group, carry):
        start = group * GROUP
        shards = [info_ref[start + index] for index in range(GROUP)]
        low_shard = high_shard = shards[0]
        reached = (shards[0] >= first) & (shards[0] <= mine)
        for shard in shards[1:]:
            low_shard = jnp.minimum(low_shard, shard)
            high_shard = jnp.maximum(high_shard, shard)
            reached = reached | ((shard >= first) & (shard <= mine))
        plain = (low_shard >= whole) & (high_shard < mine)

        @pl.when(plain)
        def _():
            update(start, False)

        @pl.when(reached & jnp.logical_not(plain))
        def _():
            update(start, True)

        return carry

    lax.fori_loop(0, at // GROUP, visit, 0)
    if last:
        mixed = acc[...] / total[...]
        for head in range(QPK):
            part = mixed[:, head * L_DEV : (head + 1) * L_DEV]
            out_ref[:, head * HEAD : (head + 1) * HEAD] = jnp.transpose(part).astype(jnp.bfloat16)


def attend(info, turned, lows, state, pieces, last):
    vmem = pl.BlockSpec(memory_space=pltpu.VMEM)
    slots = sum(piece.shape[0] for piece in pieces)
    shapes = [(HEAD, QPK * L_DEV), (1, QPK * L_DEV), (1, QPK * L_DEV)]
    if last:
        out_shape = [jax.ShapeDtypeStruct((L_DEV, QPK * HEAD), jnp.bfloat16)]
        scratch = [pltpu.VMEM(shape, jnp.float32) for shape in shapes]
    else:
        out_shape = [jax.ShapeDtypeStruct(shape, jnp.float32) for shape in shapes]
        scratch = []
    return pl.pallas_call(
        functools.partial(attend_stage, last),
        out_shape=out_shape,
        in_specs=[pl.BlockSpec(memory_space=pltpu.SMEM)]
        + [vmem] * 5
        + [pl.BlockSpec(memory_space=pl.ANY)] * len(pieces),
        out_specs=[vmem] * len(out_shape),
        scratch_shapes=scratch
        + [pltpu.VMEM((slots, L_DEV, 2 * HEAD), jnp.bfloat16), pltpu.SemaphoreType.DMA((len(pieces),))],
        compiler_params=pltpu.CompilerParams(vmem_limit_bytes=24 * 1024 * 1024),
        name="attend",
    )(info, turned, lows, *state, *pieces)


def shift(block, axis, step):
    size = lax.axis_size(axis)
    return lax.ppermute(block, axis, [(i, (i + step) % size) for i in range(size)])


Z_ORDER = (4, 3, 5, 2, 6, 1, 7)


def plane_places(z, x, core):
    rows = (z - jnp.arange(8, dtype=jnp.int32)) % 8
    stages = (((rows, 0),), ((rows, 1), (rows, 3)), ((rows[:4], 2), (rows[4:], 2)))
    return [
        jnp.concatenate([(part * 4 + (x - step) % 4) * 2 + side for side in (core, 1 - core) for part, step in own])
        for own in stages
    ]


def rope_tables(positions):
    half = HEAD // 2
    rates = jnp.exp(jnp.arange(half, dtype=jnp.float32) * (-2.0 * math.log(rope_base) / HEAD))
    angles = positions.astype(jnp.float32)[:, None] * rates[None, :]
    return jnp.cos(angles), jnp.sin(angles)


def rotate(values, tables):
    cosine, sine = (table[:, None, :] for table in tables)
    half = HEAD // 2
    first, second = values[..., :half], values[..., half:]
    return jnp.concatenate([first * cosine - second * sine, second * cosine + first * sine], axis=-1)


def per_device(
    patches,
    fc_gain,
    fc_in,
    fc_in_bias,
    fc_out,
    fc_out_bias,
    proj_weight,
    text_embed,
    frame_start,
    frame_count,
    segment_ids,
    norm_gain,
    query_weight,
    query_bias,
    key_weight,
    value_weight,
    value_bias,
):
    section = lax.axis_index("section")
    z, x, core = (lax.axis_index(name).astype(jnp.int32) for name in SEQ)
    shard = (z * 4 + x) * 2 + core
    odd = section % 2 == 1

    main_in, left_in = fold_rows(jnp.concatenate([fc_in[0], jnp.transpose(fc_out[0])], axis=1))
    own_pack = jnp.concatenate([main_in, left_in], axis=1)
    own_small = jnp.concatenate([fc_gain[0], fc_in_bias[0], fc_out_bias[0]])
    pairs = [(0, 1), (1, 0), (2, 3), (3, 2)]
    other_pack = lax.ppermute(own_pack, "section", pairs)
    other_small = lax.ppermute(own_small, "section", pairs)
    packs = [jnp.where(odd, other_pack, own_pack), jnp.where(odd, own_pack, other_pack)]
    small = jnp.stack([jnp.where(odd, other_small, own_small), jnp.where(odd, own_small, other_small)])
    sent = jnp.concatenate(
        [pack[:, :LAYER_COLS] for pack in packs] + [pack[:, LAYER_COLS:] for pack in packs], axis=1
    )
    full = lax.all_gather(sent, SEQ, axis=0, tiled=True)
    proj_full = lax.all_gather(jnp.concatenate(fold_rows(proj_weight), axis=1), SEQ, axis=0, tiled=True)

    small = jnp.concatenate(
        [feature_order(small[:, :D]), feature_order(small[:, D + FF :]), small[:, D : D + FF]], axis=1
    )

    frame = jnp.pad(patches[0], ((0, 2 * HALF_ROWS - GRID * GRID), (0, 0)))
    half = jnp.where(odd, frame[:HALF_ROWS], frame[HALF_ROWS:])
    half = jnp.dot(half, order_matrix(), preferred_element_type=jnp.float32).astype(jnp.bfloat16)
    chunks = [half[:CHUNK_ROWS], half[CHUNK_ROWS:]]

    first_row = jnp.where(section == 3, POOL, 0)
    tokens = jnp.arange(POOL * POOL // 2, dtype=jnp.int32)
    patch = jnp.arange(HALF_ROWS, dtype=jnp.int32)
    patch_row, patch_col = patch // GRID, patch % GRID
    in_cell = (patch_row[None, :] // 2 == tokens[:, None] // POOL) & (
        patch_col[None, :] // 2 == tokens[:, None] % POOL
    )
    in_cell = (in_cell & (patch_row + first_row < GRID)[None, :]).astype(jnp.bfloat16)
    tall = jnp.minimum(2, GRID - first_row - 2 * (tokens // POOL))
    wide = jnp.minimum(2, GRID - 2 * (tokens % POOL))
    area = (tall * wide).astype(jnp.float32)[:, None]

    positions = shard * L_DEV + jnp.arange(L_DEV, dtype=jnp.int32)
    own_start, own_count = frame_start[shard], frame_count[shard]
    before = jnp.maximum(shard - 1, 0)
    prev_offsets = positions - frame_start[before]
    prev_valid = (shard > 0) & (prev_offsets >= 0) & (prev_offsets < frame_count[before])
    own_valid = (positions >= own_start) & (positions < own_start + own_count)
    use_vision = (own_valid | prev_valid).astype(jnp.float32)[:, None]
    use_own = own_valid.astype(jnp.float32)[:, None]
    want = jnp.concatenate([positions, positions + L_DEV]) - own_start
    want = jnp.where((want >= 0) & (want < own_count), want, -2)[:, None]
    held = jnp.arange(4 * POOL * POOL // 2, dtype=jnp.int32) - POOL * POOL
    ids = jnp.where(held >= 0, held, -1)[None, :]

    starts = jnp.stack([jnp.sum((segment_ids < number).astype(jnp.int32)) for number in range(3)])
    mine = lax.dynamic_slice_in_dim(segment_ids, shard * L_DEV, L_DEV, 0)
    low = jnp.where(mine == 0, starts[0], jnp.where(mine == 1, starts[1], starts[2]))
    edges = jnp.stack([low[0] // L_DEV, (low[L_DEV - 1] + L_DEV - 1) // L_DEV, shard])
    info = [jnp.concatenate([places, edges]).astype(jnp.int32) for places in plane_places(z, x, core)]
    lows = jnp.tile(low, QPK)[None, :]
    tables = rope_tables(positions)

    full, small, chunks, in_cell, area, use_vision, use_own, want, ids, info, lows, tables = (
        lax.optimization_barrier(
            (full, small, chunks, in_cell, area, use_vision, use_own, want, ids, info, lows, tables)
        )
    )
    hop = [(1, 2), (0, 3)]
    ended, left = encode(chunks[0], small, full)
    passed = [lax.ppermute(ended, "section", hop)]
    (ended,) = encode(chunks[1], small, full, left)
    passed.append(lax.ppermute(ended, "section", hop))
    ended = jnp.concatenate([encode(chunk, small, full, left)[0] for chunk in passed], axis=0)
    pooled = jnp.dot(in_cell, ended, preferred_element_type=jnp.float32)
    pooled = lax.all_gather((pooled / area).astype(jnp.bfloat16), "section", tiled=True)
    picked = pick_rows(want, ids, pooled)
    arrived = lax.ppermute(picked[L_DEV:], SEQ, [(i, i + 1) for i in range(N_SEQ - 1)])
    vision = jnp.where(use_own > 0, picked[:L_DEV], arrived)
    vision, proj_full = lax.optimization_barrier((vision, proj_full))
    normed = project(vision, text_embed, use_vision, norm_gain[None, :], proj_full)

    key_heads = jnp.dot(normed, key_weight, preferred_element_type=jnp.float32)
    key_heads = rotate(key_heads[:, None, :], tables)[:, 0].astype(jnp.bfloat16)
    values = (jnp.dot(normed, value_weight, preferred_element_type=jnp.float32) + value_bias).astype(jnp.bfloat16)
    block = jnp.concatenate([key_heads, jnp.transpose(values)], axis=1)
    turned = turned_queries(normed, query_bias, tables, query_weight)
    state = [
        jnp.zeros((HEAD, QPK * L_DEV), jnp.float32),
        jnp.full((1, QPK * L_DEV), mask_floor, jnp.float32),
        jnp.zeros((1, QPK * L_DEV), jnp.float32),
    ]

    arrived = {step: shift(block, "z", step) for step in Z_ORDER}
    column = jnp.stack([block] + [arrived[step] for step in range(1, 8)])
    column, turned = lax.optimization_barrier((column, turned))
    up, down = shift(column, "x", 1), shift(column, "x", 3)
    state = attend(info[0], turned, lows, state, [column, shift(column, "core", 1)], False)
    up, down, state = lax.optimization_barrier((up, down, state))
    far_up, far_down = shift(up[:4], "x", 1), shift(down[4:], "x", 3)
    sides = [up, down, shift(up, "core", 1), shift(down, "core", 1)]
    state = attend(info[1], turned, lows, state, sides, False)
    far_up, far_down, state = lax.optimization_barrier((far_up, far_down, state))
    far = [far_up, far_down, shift(far_up, "core", 1), shift(far_down, "core", 1)]
    return attend(info[2], turned, lows, state, far, True)[0]


def solution(mesh):
    axes = ("section",) + SEQ
    parts = Mesh(mesh.devices.reshape(4, 8, 4, 2), axes)
    return jax.shard_map(
        per_device,
        mesh=parts,
        in_specs=(
            P(SEQ, None, None),
            P("section", None),
            P("section", SEQ, None),
            P("section", None),
            P("section", None, SEQ),
            P("section", None),
            P(SEQ, None),
            P(SEQ, None),
            P(),
            P(),
            P(),
            P(),
            P(None, "section"),
            P("section"),
            P(None, "section"),
            P(None, "section"),
            P("section"),
        ),
        out_specs=P(SEQ, "section"),
        check_vma=False,
    )
```
